128 devices in a mesh: frames: 16 (over x, y), tile: 8 (over z, core).
Axes of the slice: x: 4, y: 4, z: 4, core: 2. Of those that a mesh axis runs over, the one named last changes fastest.
Arguments:
- latents: bfloat16 [16, 128, 160, 256], P('frames', 'tile'), may hold values from -6 to 6
- conv_first: bfloat16 [3, 3, 256, 256], replicated, may hold values from -0.125 to 0.125
- conv_second: bfloat16 [3, 3, 256, 256], replicated, may hold values from -0.125 to 0.125
- gain_first: float32 [256], replicated, may hold values from 0.25 to 1.75
- gain_second: float32 [256], replicated, may hold values from 0.25 to 1.75
- gain_key: float32 [256], replicated, may hold values from 0.25 to 1.75
- queries: bfloat16 [8192, 2560], P(('frames', 'tile')), may hold values from -140 to 140
- key_weight: bfloat16 [256, 2560], replicated, may hold values from -0.375 to 0.375
- value_weight: bfloat16 [256, 2560], replicated, may hold values from -0.375 to 0.375
- frame_ids: int32 [16, 128], replicated, may hold values from -1 to 15, as said below
- block_ids: int32 [16, 128], replicated, may hold values from -1 to 511, as said below
- counts: int32 [16], replicated, may hold values from 1 to 128, as said below
Outputs:
- refined: bfloat16 [16, 128, 160, 256], P('frames', 'tile')
- attended: bfloat16 [8192, 2560], P(('frames', 'tile'))
The draws below stay inside these ranges and needn't reach their ends.
Inputs may be any that keep to these rules, and one draw needn't show every extreme that they name: `frame_ids`: entries j < counts[g] name frames; later entries are -1. One owner never lists two blocks that lie in the same frame and the same 16 rows of a tile. `block_ids`: entries j < counts[g] name blocks of a frame; later entries are -1. `counts`: some owner lists 128 blocks in every draw.
All inputs are finite; a program needn't handle non-finite values.
Results may differ from the reference program's by a relative error of at most 0.039.
Values may be sent and summed in bfloat16 or wider, within the bound.
No kernel may reach another device: no remote copies, remote signals or barrier semaphores. Data moves between devices by JAX's collectives and lax.ppermute only.
A program may use at most 64 MiB of HBM per device.

```python
import jax
import jax.numpy as jnp
from jax import lax

C = 256
HEADS = 20
HD = 128
W = 160
QW = 4
ROWS = 16
Q_DEV = 64
BT = 40
FRAMES = 16
RH = 128
LIST = 128
TOKENS = 8192


def list_tables(key):
    tiles = LIST // FRAMES
    per_tile = ROWS * QW
    owner_keys = jax.random.split(jax.random.fold_in(key, 11), FRAMES)

    def pick_order(owner_key):
        return jax.random.permutation(owner_key, LIST)
    sources = jax.vmap(pick_order)(owner_keys).astype(jnp.int32)
    lowest = max(1, LIST // 4)
    drawn_counts = jax.random.randint(jax.random.fold_in(key, 12), (FRAMES,), lowest, LIST + 1).astype(jnp.int32)
    fullest = jax.random.randint(jax.random.fold_in(key, 13), (), 0, FRAMES)
    drawn_counts = jnp.where(jnp.arange(FRAMES) == fullest, LIST, drawn_counts).astype(jnp.int32)
    local = jax.random.randint(jax.random.fold_in(key, 14), (FRAMES, LIST), 0, per_tile).astype(jnp.int32)
    live = jnp.arange(LIST)[None, :] < drawn_counts[:, None]
    frame_table = jnp.where(live, sources // tiles, -1).astype(jnp.int32)
    block_table = jnp.where(live, sources % tiles * per_tile + local, -1).astype(jnp.int32)
    return (frame_table, block_table, drawn_counts)


def draw_frame_ids(key, part):
    return list_tables(key)[0]


def draw_block_ids(key, part):
    return list_tables(key)[1]


def draw_counts(key, part):
    return list_tables(key)[2]


def draw_queries(key, part):
    shape = (TOKENS, HEADS * HD)
    base = jnp.clip(jax.random.normal(jax.random.fold_in(key, 24), shape, jnp.float32), -6.0, 6.0)
    return base.astype(jnp.bfloat16)


def levels(own_key, shape, pieces, low, top_value):
    def one(axis_at, shards_of):
        steps = jax.random.uniform(jax.random.fold_in(jax.random.fold_in(own_key, 6), axis_at), (shards_of,), jnp.float32, low / len(pieces), top_value / len(pieces))
        return jnp.repeat(jnp.exp(steps), shape[axis_at] // shards_of).reshape((-1,) + (1,) * (len(shape) - axis_at - 1))

    factor_of = one(*pieces[0])
    for cut in pieces[1:]:
        factor_of = factor_of * one(*cut)
    return factor_of


def bell_draw(own_key, extent, deviation, bound, shards=(), held_as=jnp.bfloat16):
    level = levels(own_key, extent, shards, -0.22, 0.18) if shards else 1.0
    result = jax.random.normal(own_key, extent, jnp.float32) * deviation * level
    return jnp.minimum(jnp.maximum(result, -bound), bound).astype(held_as)


def setup_inputs(seed: int = 0) -> dict:
    key_list = jax.random.split(jax.random.key(seed), 13)
    latents = bell_draw(key_list[0], (FRAMES, RH, W, C), 1.0, 6.0, ((0, 16), (1, 8)))
    conv_first = bell_draw(key_list[1], (3, 3, C, C), (9 * C) ** -0.5, 0.125)
    conv_second = bell_draw(key_list[2], (3, 3, C, C), (9 * C) ** -0.5, 0.125)
    gain_first = jnp.clip(1.0 + 0.15 * jax.random.normal(key_list[3], (C,), jnp.float32), 0.25, 1.75)
    gain_second = jnp.clip(1.0 + 0.15 * jax.random.normal(key_list[4], (C,), jnp.float32), 0.25, 1.75)
    gain_key = jnp.clip(1.0 + 0.15 * jax.random.normal(key_list[5], (C,), jnp.float32), 0.25, 1.75)
    queries = draw_queries(jax.random.fold_in(key_list[12], 71), 0)
    key_weight = bell_draw(key_list[7], (C, HEADS * HD), C ** -0.5, 0.375)
    value_weight = bell_draw(key_list[8], (C, HEADS * HD), C ** -0.5, 0.375)
    frame_ids = draw_frame_ids(jax.random.fold_in(key_list[12], 71), 0)
    block_ids = draw_block_ids(jax.random.fold_in(key_list[12], 71), 0)
    counts = draw_counts(jax.random.fold_in(key_list[12], 71), 0)
    return dict(latents=latents, conv_first=conv_first, conv_second=conv_second, gain_first=gain_first, gain_second=gain_second, gain_key=gain_key, queries=queries, key_weight=key_weight, value_weight=value_weight, frame_ids=frame_ids, block_ids=block_ids, counts=counts)


EPSILON = 1e-06
NEGATIVE = -1e+30

def norm_rows(values, gain):
    wide = values.astype(jnp.float32)
    mean_square = lax.optimization_barrier(jnp.mean(wide * wide, axis=-1, keepdims=True))
    return wide * lax.rsqrt(mean_square + EPSILON) * gain

def activate(values, gain):
    return jax.nn.silu(norm_rows(values, gain)).astype(jnp.bfloat16)

def convolve(padded, weight, out_rows):
    count_frames = padded.shape[0]
    width = padded.shape[2]
    channels = padded.shape[3]
    widened = jnp.pad(padded, ((0, 0), (0, 0), (1, 1), (0, 0)))
    total = jnp.zeros((count_frames * out_rows * width, channels), jnp.float32)
    for row_step in range(3):
        for col_step in range(3):
            window = widened[:, row_step:row_step + out_rows, col_step:col_step + width, :].reshape(-1, channels)
            total = total + jnp.dot(window, weight[row_step, col_step], preferred_element_type=jnp.float32)
    return total.reshape(count_frames, out_rows, width, channels)

def head_scores(keys_in, weight_pair, query_head, key_mask):
    head_dim = query_head.shape[-1]
    pair = jnp.dot(keys_in, weight_pair, preferred_element_type=jnp.float32)
    key_head = pair[:, :head_dim]
    value_head = pair[:, head_dim:]
    scale = 1.0 / head_dim ** 0.5
    scores = jnp.einsum('qd,kd->qk', query_head.astype(jnp.float32), key_head, precision=lax.Precision.HIGHEST) * scale
    scores = jnp.where(key_mask[None, :], scores, NEGATIVE)
    return (scores, value_head)

def weigh_values(weights, value_head):
    rounded = lax.optimization_barrier(weights.astype(jnp.bfloat16))
    return jnp.dot(rounded.astype(jnp.float32), value_head, precision=lax.Precision.HIGHEST)

def attend_whole(keys_in, key_mask, weight_pairs, query_heads):

    def one_head(operands):
        scores, value_head = head_scores(keys_in, operands[0], operands[1], key_mask)
        peak = lax.optimization_barrier(jnp.max(scores, axis=-1, keepdims=True))
        weights = jnp.exp(scores - peak)
        total = lax.optimization_barrier(jnp.sum(weights, axis=-1, keepdims=True))
        mixed = weigh_values(weights, value_head)
        return (mixed / total).astype(jnp.bfloat16)
    return lax.map(one_head, (weight_pairs, query_heads))

def pair_weights(key_weight, value_weight):
    channels = key_weight.shape[0]
    stacked = jnp.concatenate([key_weight.reshape(channels, HEADS, HD), value_weight.reshape(channels, HEADS, HD)], axis=-1)
    return stacked.transpose(1, 0, 2)

def reference(latents, conv_first, conv_second, gain_first, gain_second, gain_key, queries, key_weight, value_weight, frame_ids, block_ids, counts):
    row_pad = ((0, 0), (1, 1), (0, 0), (0, 0))
    first_act = activate(latents, gain_first)
    middle = (latents.astype(jnp.float32) + convolve(jnp.pad(first_act, row_pad), conv_first, RH)).astype(jnp.bfloat16)
    second_act = activate(middle, gain_second)
    refined = (middle.astype(jnp.float32) + convolve(jnp.pad(second_act, row_pad), conv_second, RH)).astype(jnp.bfloat16)
    normed = norm_rows(refined, gain_key).astype(jnp.bfloat16)
    blocks = normed.reshape(FRAMES, RH * QW, BT, C)
    weight_pairs = pair_weights(key_weight, value_weight)
    group_rows = LIST // FRAMES * Q_DEV
    slots = jnp.arange(LIST, dtype=jnp.int32)

    def owner(owner_index):
        frame_list = jnp.maximum(frame_ids[owner_index], 0).astype(jnp.int32)
        block_list = jnp.maximum(block_ids[owner_index], 0).astype(jnp.int32)
        live = slots < counts[owner_index]
        keys_in = blocks[frame_list, block_list].reshape(LIST * BT, C)
        key_mask = jnp.repeat(live, BT)
        start = (owner_index * group_rows).astype(jnp.int32)
        owner_queries = lax.dynamic_slice_in_dim(queries, start, group_rows, 0)
        query_heads = owner_queries.reshape(group_rows, HEADS, HD).transpose(1, 0, 2)
        heads_out = attend_whole(keys_in, key_mask, weight_pairs, query_heads)
        return heads_out.transpose(1, 0, 2).reshape(group_rows, HEADS * HD)
    attended = lax.map(owner, jnp.arange(FRAMES, dtype=jnp.int32)).reshape(TOKENS, HEADS * HD)
    return (refined, attended)
```

```python
import functools

import jax
import jax.numpy as jnp
from jax import lax
from jax.experimental import pallas as pl
from jax.experimental.pallas import tpu as pltpu
from jax.sharding import PartitionSpec as P

C = 256
HEADS = 20
HD = 128
QW = 4
BT = 40
W = 160
ROWS = 16
Q_DEV = 64
FRAMES = 16
TILES = 8
QROWS = HEADS * Q_DEV
EPSILON = 1e-06
NEGATIVE = -1e30
LOG2E = 1.4426950408889634
VMEM = pl.BlockSpec(memory_space=pltpu.VMEM)
SMEM = pl.BlockSpec(memory_space=pltpu.SMEM)


def normalized(wide, gain):
    mean_square = jnp.mean(wide * wide, axis=-1, keepdims=True)
    return wide * lax.rsqrt(mean_square + EPSILON) * gain


def store_windows(act, dst_ref, row):
    column = lax.broadcasted_iota(jnp.int32, act.shape, 0)
    left = jnp.where(column == 0, 0.0, pltpu.roll(act, 1, 0))
    right = jnp.where(column == W - 1, 0.0, pltpu.roll(act, W - 1, 0))
    dst_ref[row, :, 0:C] = left.astype(jnp.bfloat16)
    dst_ref[row, :, C : 2 * C] = act.astype(jnp.bfloat16)
    dst_ref[row, :, 2 * C : 3 * C] = right.astype(jnp.bfloat16)


def silu_norm(wide, half_gain):
    half = normalized(wide, half_gain)
    return half + half * jnp.tanh(half)


def windows_dot(src_ref, weight_ref, row, count):
    total = None
    for step in range(3):
        window = src_ref[row + step : row + step + count].reshape(count * W, 3 * C)
        part = jnp.dot(window, weight_ref[step], preferred_element_type=jnp.float32)
        total = part if total is None else total + part
    return total


def conv_kernel(
    pick_ref, edge_ref, x_ref, low_ref, high_ref, w1_ref, w2_ref, g1_ref, g2_ref, gk_ref,
    refined_ref, picked_ref, first_ref, middle_ref, second_ref, wide_ref,
):
    g1 = g1_ref[...] * 0.5
    g2 = g2_ref[...] * 0.5

    def first_row(source, row):
        store_windows(silu_norm(source.astype(jnp.float32), g1), first_ref, row)

    for k in range(2):
        first_row(low_ref[k], k)
        first_row(high_ref[k], ROWS + 2 + k)
    for k in range(ROWS):
        first_row(x_ref[k], k + 2)

    group = 6
    for start in range(0, ROWS + 2, group):
        total = windows_dot(first_ref, w1_ref, start, group)
        for k in range(group):
            row = start + k
            if row == 0:
                base = low_ref[1]
            elif row == ROWS + 1:
                base = high_ref[0]
            else:
                base = x_ref[row - 1]
            middle = (base.astype(jnp.float32) + total[k * W : (k + 1) * W]).astype(jnp.bfloat16)
            middle_ref[row] = middle
            act = silu_norm(middle.astype(jnp.float32), g2)
            if row == 0:
                act = act * edge_ref[0]
            if row == ROWS + 1:
                act = act * edge_ref[1]
            store_windows(act, second_ref, row)

    group = 8
    for start in range(0, ROWS, group):
        total = windows_dot(second_ref, w2_ref, start, group)
        for k in range(group):
            row = start + k
            out = middle_ref[row + 1].astype(jnp.float32) + total[k * W : (k + 1) * W]
            out = out.astype(jnp.bfloat16)
            refined_ref[row] = out
            wide_ref[row * W : (row + 1) * W] = out.astype(jnp.float32)

    gk = gk_ref[...]
    for g in range(FRAMES):
        at = pl.multiple_of(pick_ref[g] * BT, 8)
        block = normalized(wide_ref[pl.ds(at, BT)], gk)
        picked_ref[g] = block.astype(jnp.bfloat16)


def conv_call(pick, edge, latents, low, high, w1, w2, g1, g2, gk):
    return pl.pallas_call(
        conv_kernel,
        name="convs",
        out_shape=(
            jax.ShapeDtypeStruct((ROWS, W, C), jnp.bfloat16),
            jax.ShapeDtypeStruct((FRAMES, BT, C), jnp.bfloat16),
        ),
        in_specs=[SMEM, SMEM] + [VMEM] * 8,
        out_specs=(VMEM, VMEM),
        scratch_shapes=[
            pltpu.VMEM((ROWS + 4, W, 3 * C), jnp.bfloat16),
            pltpu.VMEM((ROWS + 2, W, C), jnp.bfloat16),
            pltpu.VMEM((ROWS + 2, W, 3 * C), jnp.bfloat16),
            pltpu.VMEM((ROWS * W, C), jnp.float32),
        ],
        compiler_params=pltpu.CompilerParams(vmem_limit_bytes=40 * 1024 * 1024),
        cost_estimate=pl.CostEstimate(
            flops=2 * 9 * C * C * W * (2 * ROWS + 2), bytes_accessed=6 << 20, transcendentals=0
        ),
    )(pick, edge, latents, low, high, w1, w2, g1, g2, gk)


def query_kernel(q_ref, wk_ref, high_ref, low_ref):
    scale = LOG2E / HD**0.5
    for h in range(HEADS):
        cols = slice(h * HD, (h + 1) * HD)
        turned = lax.dot_general(
            q_ref[:, cols], wk_ref[:, cols], (((1,), (1,)), ((), ())),
            preferred_element_type=jnp.float32,
        ) * scale
        high = turned.astype(jnp.bfloat16)
        high_ref[h * Q_DEV : (h + 1) * Q_DEV] = high
        low_ref[h * Q_DEV : (h + 1) * Q_DEV] = (turned - high.astype(jnp.float32)).astype(
            jnp.bfloat16
        )


def query_call(queries, key_weight):
    shape = jax.ShapeDtypeStruct((QROWS, C), jnp.bfloat16)
    return pl.pallas_call(
        query_kernel,
        name="turn_queries",
        out_shape=(shape, shape),
        in_specs=[VMEM, VMEM],
        out_specs=(VMEM, VMEM),
        compiler_params=pltpu.CompilerParams(vmem_limit_bytes=16 * 1024 * 1024),
        cost_estimate=pl.CostEstimate(
            flops=2 * QROWS * HD * C, bytes_accessed=3 << 20, transcendentals=0
        ),
    )(queries, key_weight)


BLOCK = 320
SLAB = 32


def attend_kernel(first, last, parts, *refs):
    refs = list(refs)
    qh_ref, ql_ref = refs[:2]
    x_refs = refs[2 : 2 + parts]
    bias_ref = refs[2 + parts]
    refs = refs[3 + parts :]
    if not first:
        m_in, l_in, acc_in = refs[:3]
        refs = refs[3:]
    if last:
        wv_ref, out_ref = refs[:2]
        refs = refs[2:]
    else:
        m_out, l_out, acc_out = refs[:3]
        refs = refs[3:]
    x_ref, s_ref, p_ref = refs
    tokens = x_ref.shape[0]
    at = 0
    for part in x_refs:
        size = part.shape[0] * part.shape[1]
        x_ref[at : at + size] = part[...].reshape(size, C)
        at += size
    bias = bias_ref[...]

    def scores(block, slot):
        rows = slice(block * BLOCK, (block + 1) * BLOCK)
        dims = (((1,), (1,)), ((), ()))
        s_ref[slot] = lax.dot_general(
            qh_ref[rows], x_ref[...], dims, preferred_element_type=jnp.float32
        ) + lax.dot_general(ql_ref[rows], x_ref[...], dims, preferred_element_type=jnp.float32)

    blocks = QROWS // BLOCK
    scores(0, 0)
    for block in range(blocks):
        slot = block % 2
        if block + 1 < blocks:
            scores(block + 1, 1 - slot)
        alphas = []
        sums = []
        for slab in range(BLOCK // SLAB):
            own = slice(slab * SLAB, (slab + 1) * SLAB)
            rows = slice(block * BLOCK + slab * SLAB, block * BLOCK + (slab + 1) * SLAB)
            s = s_ref[slot, own] + bias
            peak = jnp.max(s, axis=-1, keepdims=True)
            if not first:
                old = m_in[rows, 0:1]
                peak = jnp.maximum(peak, old)
                alphas.append(jnp.exp2(old - peak))
            p = jnp.exp2(s - peak)
            total = jnp.sum(p, axis=-1, keepdims=True)
            if not first:
                total = total + alphas[-1] * l_in[rows, 0:1]
            p_ref[slot, own] = p.astype(jnp.bfloat16)
            if last:
                sums.append(total)
            else:
                m_out[rows] = jnp.broadcast_to(peak, (SLAB, 128))
                l_out[rows] = jnp.broadcast_to(total, (SLAB, 128))
        rows = slice(block * BLOCK, (block + 1) * BLOCK)
        mixed = jnp.dot(p_ref[slot], x_ref[...], preferred_element_type=jnp.float32)
        if not first:
            mixed = mixed + jnp.concatenate(alphas, 0) * acc_in[rows]
        if not last:
            acc_out[rows] = mixed
        else:
            mixed = mixed / jnp.concatenate(sums, 0)
            high = mixed.astype(jnp.bfloat16)
            low = (mixed - high.astype(jnp.float32)).astype(jnp.bfloat16)
            for k in range(BLOCK // Q_DEV):
                h = block * (BLOCK // Q_DEV) + k
                cols = slice(h * HD, (h + 1) * HD)
                own = slice(k * Q_DEV, (k + 1) * Q_DEV)
                both = jnp.concatenate([high[own], low[own]], 0)
                value = jnp.dot(both, wv_ref[:, cols], preferred_element_type=jnp.float32)
                out_ref[:, cols] = (value[:Q_DEV] + value[Q_DEV:]).astype(jnp.bfloat16)


def attend_call(qh, ql, parts, bias, state=None, value_weight=None):
    first = state is None
    last = value_weight is not None
    tokens = sum(part.shape[0] * part.shape[1] for part in parts)
    operands = [qh, ql, *parts, bias]
    aliases = {}
    if not first:
        if not last:
            aliases = {len(operands) + k: k for k in range(3)}
        operands += list(state)
    if last:
        operands.append(value_weight)
        out_shape = jax.ShapeDtypeStruct((Q_DEV, HEADS * HD), jnp.bfloat16)
        out_specs = VMEM
    else:
        stat = jax.ShapeDtypeStruct((QROWS, 128), jnp.float32)
        out_shape = (stat, stat, jax.ShapeDtypeStruct((QROWS, C), jnp.float32))
        out_specs = (VMEM, VMEM, VMEM)
    return pl.pallas_call(
        functools.partial(attend_kernel, first, last, len(parts)),
        name="attend",
        out_shape=out_shape,
        in_specs=[VMEM] * len(operands),
        out_specs=out_specs,
        input_output_aliases=aliases,
        scratch_shapes=[
            pltpu.VMEM((tokens, C), jnp.bfloat16),
            pltpu.VMEM((2, BLOCK, tokens), jnp.float32),
            pltpu.VMEM((2, BLOCK, tokens), jnp.bfloat16),
        ],
        compiler_params=pltpu.CompilerParams(vmem_limit_bytes=40 * 1024 * 1024),
        cost_estimate=pl.CostEstimate(
            flops=6 * QROWS * C * tokens, bytes_accessed=6 << 20, transcendentals=QROWS * tokens
        ),
    )(*operands)


def core_swap(x):
    return lax.ppermute(x, "tile", [(t, t ^ 1) for t in range(TILES)])


def turn(x, by):
    pairs = [(t, 2 * ((t // 2 + by) % 4) + t % 2) for t in range(TILES)]
    return lax.ppermute(x, "tile", pairs)


def local(
    latents, conv_first, conv_second, gain_first, gain_second, gain_key,
    queries, key_weight, value_weight, frame_ids, block_ids, counts,
):
    tile = lax.axis_index("tile")
    frame = lax.axis_index("frames")
    forward = [(i, i + 1) for i in range(TILES - 1)]
    backward = [(i + 1, i) for i in range(TILES - 1)]
    own = latents[0]
    low = lax.ppermute(own[ROWS - 2 :], "tile", forward)
    high = lax.ppermute(own[:2], "tile", backward)

    slots = jnp.arange(frame_ids.shape[1], dtype=jnp.int32)
    live = slots[None, :] < counts[:, None]
    per_tile = ROWS * QW
    local_id = block_ids - tile * per_tile
    hit = live & (frame_ids == frame) & (local_id >= 0) & (local_id < per_tile)
    pick = jnp.sum(jnp.where(hit, local_id, 0), axis=1, dtype=jnp.int32)
    edge = jnp.stack([tile > 0, tile < TILES - 1]).astype(jnp.float32)

    depth, core = tile // 2, tile % 2
    order = []
    for by in (0, -1, 1):
        z = (depth + by) % 4
        order += [2 * z + core, 2 * z + 1 - core]
    order = [order[0], order[1], order[2], order[4], order[3], order[5]]
    z = (depth + 2) % 4
    order = jnp.stack(order + [2 * z + core, 2 * z + 1 - core])
    own_live = live[frame]
    own_frames = frame_ids[frame]
    own_tiles = block_ids[frame] // per_tile
    there = (
        own_live[None, None, :]
        & (own_frames[None, None, :] == jnp.arange(FRAMES, dtype=jnp.int32)[None, :, None])
        & (own_tiles[None, None, :] == order[:, None, None])
    ).any(-1)
    bias = jnp.where(there, 0.0, NEGATIVE).astype(jnp.float32)
    bias = jnp.repeat(bias, BT, axis=1).reshape(4, 1, 2 * FRAMES * BT)

    qh, ql = query_call(queries, key_weight)
    refined, picked = conv_call(
        pick, edge, own, low, high,
        conv_first.reshape(3, 3 * C, C), conv_second.reshape(3, 3 * C, C),
        gain_first[None], gain_second[None], gain_key[None],
    )
    mine = lax.all_to_all(picked, "frames", split_axis=0, concat_axis=0, tiled=True)
    partner = core_swap(mine)
    below = turn(mine, 1)
    above = turn(mine, -1)
    half = FRAMES // 2
    far_low = turn(below[:half], 1)
    far_high = turn(above[half:], -1)
    below_swap = core_swap(below)
    above_swap = core_swap(above)
    far_low_swap = core_swap(far_low)
    far_high_swap = core_swap(far_high)
    state = attend_call(qh, ql, (mine, partner), bias[0])
    state = attend_call(qh, ql, (below, above), bias[1], state)
    state = attend_call(qh, ql, (below_swap, above_swap), bias[2], state)
    attended = attend_call(
        qh, ql, (far_low, far_high, far_low_swap, far_high_swap), bias[3], state, value_weight
    )
    return (refined[None], attended)


def solution(mesh):
    in_specs = (
        P("frames", "tile", None, None),
        P(), P(), P(), P(), P(),
        P(("frames", "tile"), None),
        P(), P(), P(), P(), P(),
    )
    out_specs = (P("frames", "tile", None, None), P(("frames", "tile"), None))
    return jax.shard_map(local, mesh=mesh, in_specs=in_specs, out_specs=out_specs, check_vma=False)
```

```python
import functools

import jax
import jax.numpy as jnp
from jax import lax
from jax.experimental import pallas as pl
from jax.experimental.pallas import tpu as pltpu
from jax.sharding import PartitionSpec as P

C = 256
HEADS = 20
HD = 128
QW = 4
BT = 40
W = 160
ROWS = 16
Q_DEV = 64
FRAMES = 16
TILES = 8
QROWS = HEADS * Q_DEV
EPSILON = 1e-06
NEGATIVE = -1e30
LOG2E = 1.4426950408889634
VMEM = pl.BlockSpec(memory_space=pltpu.VMEM)
SMEM = pl.BlockSpec(memory_space=pltpu.SMEM)


def normalized(wide, gain):
    mean_square = jnp.mean(wide * wide, axis=-1, keepdims=True)
    return wide * lax.rsqrt(mean_square + EPSILON) * gain


def store_windows(act, dst_ref, row):
    column = lax.broadcasted_iota(jnp.int32, (8, C), 0)
    left = pltpu.roll(act, 1, 0)
    left = jnp.concatenate([jnp.where(column == 0, 0.0, left[:8]), left[8:]], 0)
    right = pltpu.roll(act, W - 1, 0)
    right = jnp.concatenate([right[: W - 8], jnp.where(column == 7, 0.0, right[W - 8 :])], 0)
    dst_ref[row, :, 0:C] = left.astype(jnp.bfloat16)
    dst_ref[row, :, C : 2 * C] = act.astype(jnp.bfloat16)
    dst_ref[row, :, 2 * C : 3 * C] = right.astype(jnp.bfloat16)


def silu_norm(wide, half_gain):
    half = normalized(wide, half_gain)
    return half + half * jnp.tanh(half)


def dot_rows(windows, weight_ref):
    total = None
    for step, window in enumerate(windows):
        part = jnp.dot(
            window.reshape(-1, 3 * C), weight_ref[step], preferred_element_type=jnp.float32
        )
        total = part if total is None else total + part
    return total


INNER = ROWS - 2


def inner_kernel(
    x_hbm, w1_hbm, w2_hbm, g1_hbm, g2_hbm, gk_hbm, frames_hbm, blocks_hbm,
    second_ref, middle_ref, sides_ref, base_ref, w1_ref, w2_ref,
    g1_ref, g2_ref, gk_ref, frames_ref, blocks_ref,
    x_ref, first_ref, sems,
):
    chunk = ROWS // 4
    pairs = [(g1_hbm, g1_ref), (g2_hbm, g2_ref)]
    for k in range(4):
        own = pl.ds(k * chunk, chunk)
        pairs.append((x_hbm.at[own], x_ref.at[own]))
    pairs += [
        (w1_hbm, w1_ref), (w2_hbm, w2_ref), (gk_hbm, gk_ref),
        (frames_hbm, frames_ref), (blocks_hbm, blocks_ref),
    ]
    copies = [
        pltpu.make_async_copy(src, dst, sems.at[k]) for k, (src, dst) in enumerate(pairs)
    ]
    for copy in copies:
        copy.start()
    copies[0].wait()
    copies[1].wait()
    g1 = g1_ref[...] * 0.5
    g2 = g2_ref[...] * 0.5

    def first_rows(rows):
        for row in rows:
            store_windows(silu_norm(x_ref[row].astype(jnp.float32), g1), first_ref, row)

    def middle_rows(rows):
        start, count = rows[0], len(rows)
        return dot_rows(
            [first_ref[start + step : start + step + count] for step in range(3)], w1_ref
        )

    def second_rows(rows, total):
        for k, row in enumerate(rows):
            middle = x_ref[row + 1].astype(jnp.float32) + total[k * W : (k + 1) * W]
            middle_ref[row] = middle.astype(jnp.bfloat16)
            store_windows(silu_norm(middle, g2), second_ref, row)

    copies[2].wait()
    first_rows(range(0, chunk))
    for copy in copies[3:]:
        copy.wait()
    first_rows(range(chunk, 7))
    parts = [range(0, 5), range(5, 10), range(10, INNER)]
    totals = [middle_rows(parts[0])]
    first_rows(range(7, 12))
    totals.append(middle_rows(parts[1]))
    first_rows(range(12, ROWS))
    second_rows(parts[0], totals[0])
    totals.append(middle_rows(parts[2]))
    for k in range(2):
        sides_ref[k] = first_ref[k]
        sides_ref[2 + k] = first_ref[ROWS - 2 + k]
        base_ref[k] = x_ref[k * (ROWS - 1)]
    second_rows(parts[1], totals[1])
    second_rows(parts[2], totals[2])


def inner_call(latents, w1, w2, g1, g2, gk, frame_ids, block_ids):
    weight = jax.ShapeDtypeStruct((3, 3 * C, C), jnp.bfloat16)
    gain = jax.ShapeDtypeStruct((1, C), jnp.float32)
    table = jax.ShapeDtypeStruct(frame_ids.shape, jnp.int32)
    out_shape = (
        jax.ShapeDtypeStruct((INNER, W, 3 * C), jnp.bfloat16),
        jax.ShapeDtypeStruct((INNER, W, C), jnp.bfloat16),
        jax.ShapeDtypeStruct((4, W, 3 * C), jnp.bfloat16),
        jax.ShapeDtypeStruct((2, W, C), jnp.bfloat16),
        weight, weight, gain, gain, gain, table, table,
    )
    return pl.pallas_call(
        inner_kernel,
        name="inner_rows",
        out_shape=out_shape,
        in_specs=[pl.BlockSpec(memory_space=pltpu.HBM)] * 8,
        out_specs=(VMEM,) * len(out_shape),
        scratch_shapes=[
            pltpu.VMEM((ROWS, W, C), jnp.bfloat16),
            pltpu.VMEM((ROWS, W, 3 * C), jnp.bfloat16),
            pltpu.SemaphoreType.DMA((11,)),
        ],
        compiler_params=pltpu.CompilerParams(vmem_limit_bytes=28 * 1024 * 1024),
        cost_estimate=pl.CostEstimate(
            flops=2 * 9 * C * C * W * INNER, bytes_accessed=4 << 20, transcendentals=0
        ),
    )(latents, w1, w2, g1, g2, gk, frame_ids, block_ids)


def outer_kernel(
    near_ref, away_ref, inner_ref, middle_ref, sides_ref, base_ref, w1_ref, w2_ref,
    g1_ref, g2_ref, gk_ref, frames_ref, blocks_ref,
    refined_hbm, picked_ref,
    refined_ref, first_ref, side_middle_ref, second_ref, wide_ref, sems,
):
    frame = lax.axis_index("frames")
    tile = lax.axis_index("tile")
    north = lax.rem(tile, 2) == 1
    half = (ROWS - 4) // 2
    total = dot_rows([inner_ref[step : step + half] for step in range(3)], w2_ref)

    per_tile = ROWS * QW
    own = blocks_ref[...] - tile * per_tile
    hit = (frames_ref[...] == frame) & (own >= 0) & (own < per_tile)
    found = jnp.where(hit, own, 0).astype(jnp.float32)
    picks = [jnp.max(found[g : g + 1]).astype(jnp.int32) for g in range(FRAMES)]

    def second_rows(total, rows):
        for k, row in enumerate(rows):
            if 0 < row < ROWS - 1:
                base = middle_ref[row - 1]
            else:
                base = side_middle_ref[1 if row == 0 else 2]
            out = base.astype(jnp.float32) + total[k * W : (k + 1) * W]
            out = out.astype(jnp.bfloat16)
            refined_ref[row] = out
            wide_ref[row * W : (row + 1) * W] = out.astype(jnp.float32)

    def send(k, start, count):
        rows = pl.ds(start, count)
        copy = pltpu.make_async_copy(refined_ref.at[rows], refined_hbm.at[rows], sems.at[k])
        copy.start()
        return copy

    g1 = g1_ref[...] * 0.5
    g2 = g2_ref[...] * 0.5
    low, high = [], []
    for k in range(2):
        near = near_ref[k].astype(jnp.float32)
        away = away_ref[k].astype(jnp.float32)
        low.append(jnp.where(north, near, away))
        high.append(jnp.where(north, away, near))
    for k in range(2):
        store_windows(silu_norm(low[k], g1), first_ref, k)
        first_ref[2 + k] = sides_ref[k]
        first_ref[4 + k] = sides_ref[2 + k]
        store_windows(silu_norm(high[k], g1), first_ref, 6 + k)
        second_ref[2 + k] = inner_ref[k]
        second_ref[4 + k] = inner_ref[INNER - 2 + k]
    edges = dot_rows(
        [
            jnp.concatenate([first_ref[step : step + 2], first_ref[4 + step : 6 + step]], 0)
            for step in range(3)
        ],
        w1_ref,
    )
    second_rows(total, range(2, 2 + half))
    total = dot_rows([inner_ref[half + step : 2 * half + step] for step in range(3)], w2_ref)

    bases = [low[1], base_ref[0].astype(jnp.float32), base_ref[1].astype(jnp.float32), high[0]]
    places = [0, 1, 6, 7]
    for k in range(4):
        middle = bases[k] + edges[k * W : (k + 1) * W]
        act = silu_norm(middle, g2)
        if k == 0:
            act = jnp.where(tile > 0, act, 0.0)
        if k == 3:
            act = jnp.where(tile < TILES - 1, act, 0.0)
        side_middle_ref[k] = middle.astype(jnp.bfloat16)
        store_windows(act, second_ref, places[k])
    edges = dot_rows(
        [
            jnp.concatenate([second_ref[step : step + 2], second_ref[4 + step : 6 + step]], 0)
            for step in range(3)
        ],
        w2_ref,
    )
    second_rows(total, range(2 + half, ROWS - 2))
    second_rows(edges, [0, 1, ROWS - 2, ROWS - 1])
    copy = send(0, 0, ROWS)

    gk = gk_ref[...]
    for g in range(FRAMES):
        at = pl.multiple_of(picks[g] * BT, 8)
        block = normalized(wide_ref[pl.ds(at, BT)], gk)
        picked_ref[g] = block.astype(jnp.bfloat16)
    copy.wait()


def outer_call(near, away, inner):
    return pl.pallas_call(
        outer_kernel,
        name="outer_rows",
        out_shape=(
            jax.ShapeDtypeStruct((ROWS, W, C), jnp.bfloat16),
            jax.ShapeDtypeStruct((FRAMES, BT, C), jnp.bfloat16),
        ),
        in_specs=[VMEM] * 13,
        out_specs=(pl.BlockSpec(memory_space=pltpu.HBM), VMEM),
        scratch_shapes=[
            pltpu.VMEM((ROWS, W, C), jnp.bfloat16),
            pltpu.VMEM((8, W, 3 * C), jnp.bfloat16),
            pltpu.VMEM((4, W, C), jnp.bfloat16),
            pltpu.VMEM((8, W, 3 * C), jnp.bfloat16),
            pltpu.VMEM((ROWS * W, C), jnp.float32),
            pltpu.SemaphoreType.DMA((1,)),
        ],
        compiler_params=pltpu.CompilerParams(vmem_limit_bytes=28 * 1024 * 1024),
        cost_estimate=pl.CostEstimate(
            flops=2 * 9 * C * C * W * (ROWS + 4), bytes_accessed=4 << 20, transcendentals=0
        ),
    )(near, away, *inner)


def query_kernel(q_ref, wk_ref, frames_ref, blocks_ref, high_ref, low_ref, bias_ref):
    frame = lax.axis_index("frames")
    tile = lax.axis_index("tile")
    per_tile = ROWS * QW
    row = lax.broadcasted_iota(jnp.int32, frames_ref.shape, 0)
    source = frames_ref[...] * TILES + lax.shift_right_arithmetic(blocks_ref[...], 6)
    source = jnp.where((row == frame) & (frames_ref[...] >= 0), source, -1)
    source = jnp.max(source.astype(jnp.float32), axis=0, keepdims=True)
    sources = FRAMES * TILES
    number = lax.broadcasted_iota(jnp.int32, (sources, source.shape[1]), 0).astype(jnp.float32)
    listed = jnp.max(jnp.where(source == number, 1.0, 0.0), axis=1, keepdims=True)
    tokens = FRAMES * BT
    place = lax.broadcasted_iota(jnp.int32, (sources, tokens), 1)
    of_frame = lax.shift_right_logical(place * 205, 13)
    number = lax.broadcasted_iota(jnp.int32, (sources, tokens), 0)
    wide = jnp.broadcast_to(listed, (sources, tokens))
    depth, core = lax.div(tile, 2), lax.rem(tile, 2)
    odd = lax.rem(depth, 2) == 1
    even_side = jnp.where(odd, depth - 1, depth + 1)
    odd_side = lax.rem(jnp.where(odd, depth + 1, depth + 3), 4)
    planes = {"own": depth, "x": even_side, "y": odd_side, "far": lax.rem(depth + 2, 4)}
    for k, (plane, other) in enumerate(ORDER):
        at = 2 * planes[plane] + (1 - core if other else core)
        match = jnp.where(number == of_frame * TILES + at, wide, 0.0)
        there = jnp.max(match, axis=0, keepdims=True)
        bias_ref[k : k + 1] = jnp.where(there > 0.5, 0.0, NEGATIVE)

    scale = LOG2E / HD**0.5
    for h in range(HEADS):
        cols = slice(h * HD, (h + 1) * HD)
        turned = lax.dot_general(
            q_ref[:, cols], wk_ref[:, cols], (((1,), (1,)), ((), ())),
            preferred_element_type=jnp.float32,
        ) * scale
        high = turned.astype(jnp.bfloat16)
        high_ref[h * Q_DEV : (h + 1) * Q_DEV] = high
        low_ref[h * Q_DEV : (h + 1) * Q_DEV] = (turned - high.astype(jnp.float32)).astype(
            jnp.bfloat16
        )


ORDER = (
    ("own", 0), ("own", 1), ("x", 0), ("y", 0), ("x", 1), ("y", 1), ("far", 0), ("far", 1),
)


def query_call(queries, key_weight, frame_ids, block_ids):
    shape = jax.ShapeDtypeStruct((QROWS, C), jnp.bfloat16)
    return pl.pallas_call(
        query_kernel,
        name="turn_queries",
        out_shape=(shape, shape, jax.ShapeDtypeStruct((TILES, FRAMES * BT), jnp.float32)),
        in_specs=[VMEM] * 4,
        out_specs=(VMEM,) * 3,
        compiler_params=pltpu.CompilerParams(vmem_limit_bytes=16 * 1024 * 1024),
        cost_estimate=pl.CostEstimate(
            flops=2 * QROWS * HD * C, bytes_accessed=3 << 20, transcendentals=0
        ),
    )(queries, key_weight, frame_ids, block_ids)


BLOCK = 320
SLAB = 32


def attend_kernel(first, last, parts, chunk, *refs):
    refs = list(refs)
    qh_ref, ql_ref = refs[:2]
    x_refs = refs[2 : 2 + parts]
    bias_ref = refs[2 + parts]
    refs = refs[3 + parts :]
    if not first:
        m_in, l_in, acc_in = refs[:3]
        refs = refs[3:]
    if last:
        wv_ref, out_ref = refs[:2]
        refs = refs[2:]
    else:
        m_out, l_out, acc_out = refs[:3]
        refs = refs[3:]
    x_ref, s_ref, p_ref = refs
    tokens = x_ref.shape[0]
    at = 0
    for part in x_refs:
        size = part.shape[0] * part.shape[1]
        x_ref[at : at + size] = part[...].reshape(size, C)
        at += size
    bias = jnp.concatenate([bias_ref[2 * chunk : 2 * chunk + 1], bias_ref[2 * chunk + 1 : 2 * chunk + 2]], 1)

    def scores(block, slot):
        rows = slice(block * BLOCK, (block + 1) * BLOCK)
        dims = (((1,), (1,)), ((), ()))
        s_ref[slot] = lax.dot_general(
            qh_ref[rows], x_ref[...], dims, preferred_element_type=jnp.float32
        ) + lax.dot_general(ql_ref[rows], x_ref[...], dims, preferred_element_type=jnp.float32)

    blocks = QROWS // BLOCK
    scores(0, 0)
    for block in range(blocks):
        slot = block % 2
        if block + 1 < blocks:
            scores(block + 1, 1 - slot)
        alphas = []
        sums = []
        for slab in range(BLOCK // SLAB):
            own = slice(slab * SLAB, (slab + 1) * SLAB)
            rows = slice(block * BLOCK + slab * SLAB, block * BLOCK + (slab + 1) * SLAB)
            s = s_ref[slot, own] + bias
            peak = jnp.max(s, axis=-1, keepdims=True)
            if not first:
                old = m_in[rows, 0:1]
                peak = jnp.maximum(peak, old)
                alphas.append(jnp.exp2(old - peak))
            p = jnp.exp2(s - peak)
            total = jnp.sum(p, axis=-1, keepdims=True)
            if not first:
                total = total + alphas[-1] * l_in[rows, 0:1]
            p_ref[slot, own] = p.astype(jnp.bfloat16)
            if last:
                sums.append(total)
            else:
                m_out[rows] = jnp.broadcast_to(peak, (SLAB, 128))
                l_out[rows] = jnp.broadcast_to(total, (SLAB, 128))
        rows = slice(block * BLOCK, (block + 1) * BLOCK)
        mixed = jnp.dot(p_ref[slot], x_ref[...], preferred_element_type=jnp.float32)
        if not first:
            mixed = mixed + jnp.concatenate(alphas, 0) * acc_in[rows]
        if not last:
            acc_out[rows] = mixed
        else:
            mixed = mixed / jnp.concatenate(sums, 0)
            high = mixed.astype(jnp.bfloat16)
            low = (mixed - high.astype(jnp.float32)).astype(jnp.bfloat16)
            for k in range(BLOCK // Q_DEV):
                h = block * (BLOCK // Q_DEV) + k
                cols = slice(h * HD, (h + 1) * HD)
                own = slice(k * Q_DEV, (k + 1) * Q_DEV)
                both = jnp.concatenate([high[own], low[own]], 0)
                value = jnp.dot(both, wv_ref[:, cols], preferred_element_type=jnp.float32)
                out_ref[:, cols] = (value[:Q_DEV] + value[Q_DEV:]).astype(jnp.bfloat16)


def attend_call(qh, ql, parts, bias, chunk, state=None, value_weight=None):
    first = state is None
    last = value_weight is not None
    tokens = sum(part.shape[0] * part.shape[1] for part in parts)
    operands = [qh, ql, *parts, bias]
    aliases = {}
    if not first:
        if not last:
            aliases = {len(operands) + k: k for k in range(3)}
        operands += list(state)
    if last:
        operands.append(value_weight)
        out_shape = jax.ShapeDtypeStruct((Q_DEV, HEADS * HD), jnp.bfloat16)
        out_specs = VMEM
    else:
        stat = jax.ShapeDtypeStruct((QROWS, 128), jnp.float32)
        out_shape = (stat, stat, jax.ShapeDtypeStruct((QROWS, C), jnp.float32))
        out_specs = (VMEM, VMEM, VMEM)
    return pl.pallas_call(
        functools.partial(attend_kernel, first, last, len(parts), chunk),
        name="attend",
        out_shape=out_shape,
        in_specs=[VMEM] * len(operands),
        out_specs=out_specs,
        input_output_aliases=aliases,
        scratch_shapes=[
            pltpu.VMEM((tokens, C), jnp.bfloat16),
            pltpu.VMEM((2, BLOCK, tokens), jnp.float32),
            pltpu.VMEM((2, BLOCK, tokens), jnp.bfloat16),
        ],
        compiler_params=pltpu.CompilerParams(vmem_limit_bytes=40 * 1024 * 1024),
        cost_estimate=pl.CostEstimate(
            flops=6 * QROWS * C * tokens, bytes_accessed=6 << 20, transcendentals=QROWS * tokens
        ),
    )(*operands)


def core_swap(x):
    return lax.ppermute(x, "tile", [(t, t ^ 1) for t in range(TILES)])


def partner_plane(z, odd):
    return z ^ 1 if not odd else ((z + 1) % 4 if z % 2 else (z + 3) % 4)


def plane_swap(x, odds):
    pairs = [(t, 2 * partner_plane(t // 2, odds[t % 2]) + t % 2) for t in range(TILES)]
    return lax.ppermute(x, "tile", pairs)


def local(
    latents, conv_first, conv_second, gain_first, gain_second, gain_key,
    queries, key_weight, value_weight, frame_ids, block_ids, counts,
):
    core = lax.rem(lax.axis_index("tile"), 2)
    own = latents[0]
    near = lax.dynamic_slice_in_dim(own, (ROWS - 2) * (1 - core), 2, 0)
    away = lax.dynamic_slice_in_dim(own, (ROWS - 2) * core, 2, 0)
    near = core_swap(near)
    across = [(t, t + 1 if t % 2 else t - 1) for t in range(1, TILES - 1)]
    away = lax.ppermute(away, "tile", across)

    stay = functools.partial(pltpu.with_memory_space_constraint, memory_space=pltpu.HBM)
    inner = inner_call(
        stay(own),
        stay(conv_first.reshape(3, 3 * C, C)), stay(conv_second.reshape(3, 3 * C, C)),
        stay(gain_first[None]), stay(gain_second[None]), stay(gain_key[None]),
        stay(frame_ids), stay(block_ids),
    )
    refined, picked = outer_call(near, away, inner)
    qh, ql, bias = query_call(queries, key_weight, inner[9], inner[10])
    mine = lax.all_to_all(picked, "frames", split_axis=0, concat_axis=0, tiled=True)
    partner = core_swap(mine)
    even_side = plane_swap(mine, (False, False))
    odd_side = plane_swap(mine, (True, True))
    state = attend_call(qh, ql, (mine, partner), bias, 0)
    even_side, odd_side, state = lax.optimization_barrier((even_side, odd_side, state))
    far = plane_swap(jnp.where(core == 0, even_side, odd_side), (True, False))
    even_swap = core_swap(even_side)
    odd_swap = core_swap(odd_side)
    state = attend_call(qh, ql, (even_side, odd_side), bias, 1, state)
    far, state = lax.optimization_barrier((far, state))
    far_swap = core_swap(far)
    state = attend_call(qh, ql, (even_swap, odd_swap), bias, 2, state)
    attended = attend_call(qh, ql, (far, far_swap), bias, 3, state, value_weight)
    return (refined[None], attended)


def solution(mesh):
    in_specs = (
        P("frames", "tile", None, None),
        P(), P(), P(), P(), P(),
        P(("frames", "tile"), None),
        P(), P(), P(), P(), P(),
    )
    out_specs = (P("frames", "tile", None, None), P(("frames", "tile"), None))
    return jax.shard_map(local, mesh=mesh, in_specs=in_specs, out_specs=out_specs, check_vma=False)
```

```python
import functools

import jax
import jax.numpy as jnp
from jax import lax
from jax.experimental import pallas as pl
from jax.experimental.pallas import tpu as pltpu
from jax.sharding import PartitionSpec as P

C = 256
HEADS = 20
HD = 128
QW = 4
BT = 40
W = 160
ROWS = 16
Q_DEV = 64
FRAMES = 16
TILES = 8
QROWS = HEADS * Q_DEV
EPSILON = 1e-06
NEGATIVE = -1e30
LOG2E = 1.4426950408889634
VMEM = pl.BlockSpec(memory_space=pltpu.VMEM)
SMEM = pl.BlockSpec(memory_space=pltpu.SMEM)


def normalized(wide, gain):
    mean_square = jnp.mean(wide * wide, axis=-1, keepdims=True)
    return wide * lax.rsqrt(mean_square + EPSILON) * gain


def store_windows(act, dst_ref, row):
    column = lax.broadcasted_iota(jnp.int32, (8, C), 0)
    left = pltpu.roll(act, 1, 0)
    left = jnp.concatenate([jnp.where(column == 0, 0.0, left[:8]), left[8:]], 0)
    right = pltpu.roll(act, W - 1, 0)
    right = jnp.concatenate([right[: W - 8], jnp.where(column == 7, 0.0, right[W - 8 :])], 0)
    dst_ref[row, :, 0:C] = left.astype(jnp.bfloat16)
    dst_ref[row, :, C : 2 * C] = act.astype(jnp.bfloat16)
    dst_ref[row, :, 2 * C : 3 * C] = right.astype(jnp.bfloat16)


def silu_norm(wide, half_gain):
    half = normalized(wide, half_gain)
    return half + half * jnp.tanh(half)


def dot_rows(windows, weight_ref):
    total = None
    for step, window in enumerate(windows):
        part = jnp.dot(
            window.reshape(-1, 3 * C), weight_ref[step], preferred_element_type=jnp.float32
        )
        total = part if total is None else total + part
    return total


INNER = ROWS - 2


def inner_kernel(
    x_hbm, w1_hbm, w2_hbm, g1_hbm, g2_hbm, gk_hbm, frames_hbm, blocks_hbm,
    second_ref, middle_ref, sides_ref, base_ref, w1_ref, w2_ref,
    g1_ref, g2_ref, gk_ref, frames_ref, blocks_ref,
    x_ref, first_ref, sems,
):
    chunk = ROWS // 4
    pairs = [(g1_hbm, g1_ref), (g2_hbm, g2_ref)]
    for k in range(4):
        own = pl.ds(k * chunk, chunk)
        pairs.append((x_hbm.at[own], x_ref.at[own]))
    pairs += [
        (w1_hbm, w1_ref), (w2_hbm, w2_ref), (gk_hbm, gk_ref),
        (frames_hbm, frames_ref), (blocks_hbm, blocks_ref),
    ]
    copies = [
        pltpu.make_async_copy(src, dst, sems.at[k]) for k, (src, dst) in enumerate(pairs)
    ]
    for k in (2, 0, 3, 4, 5, 1, 6):
        copies[k].start()
    copies[0].wait()
    g1 = g1_ref[...] * 0.5

    def first_rows(rows):
        for row in rows:
            store_windows(silu_norm(x_ref[row].astype(jnp.float32), g1), first_ref, row)

    def middle_rows(rows):
        start, count = rows[0], len(rows)
        return dot_rows(
            [first_ref[start + step : start + step + count] for step in range(3)], w1_ref
        )

    def second_rows(rows, total, g2):
        for k, row in enumerate(rows):
            middle = x_ref[row + 1].astype(jnp.float32) + total[k * W : (k + 1) * W]
            middle_ref[row] = middle.astype(jnp.bfloat16)
            store_windows(silu_norm(middle, g2), second_ref, row)

    copies[2].wait()
    first_rows(range(0, chunk))
    for k in (3, 4, 5, 1, 6):
        copies[k].wait()
    later = copies[7:]
    for copy in later:
        copy.start()
    g2 = g2_ref[...] * 0.5
    first_rows(range(chunk, 7))
    parts = [range(0, 5), range(5, 10), range(10, INNER)]
    totals = [middle_rows(parts[0])]
    first_rows(range(7, 12))
    totals.append(middle_rows(parts[1]))
    first_rows(range(12, ROWS))
    second_rows(parts[0], totals[0], g2)
    totals.append(middle_rows(parts[2]))
    for k in range(2):
        sides_ref[k] = first_ref[k]
        sides_ref[2 + k] = first_ref[ROWS - 2 + k]
        base_ref[k] = x_ref[k * (ROWS - 1)]
    second_rows(parts[1], totals[1], g2)
    second_rows(parts[2], totals[2], g2)
    for copy in later:
        copy.wait()


def inner_call(latents, w1, w2, g1, g2, gk, frame_ids, block_ids):
    weight = jax.ShapeDtypeStruct((3, 3 * C, C), jnp.bfloat16)
    gain = jax.ShapeDtypeStruct((1, C), jnp.float32)
    table = jax.ShapeDtypeStruct(frame_ids.shape, jnp.int32)
    out_shape = (
        jax.ShapeDtypeStruct((INNER, W, 3 * C), jnp.bfloat16),
        jax.ShapeDtypeStruct((INNER, W, C), jnp.bfloat16),
        jax.ShapeDtypeStruct((4, W, 3 * C), jnp.bfloat16),
        jax.ShapeDtypeStruct((2, W, C), jnp.bfloat16),
        weight, weight, gain, gain, gain, table, table,
    )
    return pl.pallas_call(
        inner_kernel,
        name="inner_rows",
        out_shape=out_shape,
        in_specs=[pl.BlockSpec(memory_space=pltpu.HBM)] * 8,
        out_specs=(VMEM,) * len(out_shape),
        scratch_shapes=[
            pltpu.VMEM((ROWS, W, C), jnp.bfloat16),
            pltpu.VMEM((ROWS, W, 3 * C), jnp.bfloat16),
            pltpu.SemaphoreType.DMA((11,)),
        ],
        compiler_params=pltpu.CompilerParams(vmem_limit_bytes=28 * 1024 * 1024),
        cost_estimate=pl.CostEstimate(
            flops=2 * 9 * C * C * W * INNER, bytes_accessed=4 << 20, transcendentals=0
        ),
    )(latents, w1, w2, g1, g2, gk, frame_ids, block_ids)


def outer_kernel(
    near_ref, away_ref, inner_ref, middle_ref, sides_ref, base_ref, w1_ref, w2_ref,
    g1_ref, g2_ref, gk_ref, frames_ref, blocks_ref,
    refined_hbm, picked_ref,
    refined_ref, first_ref, side_middle_ref, second_ref, wide_ref, sems,
):
    frame = lax.axis_index("frames")
    tile = lax.axis_index("tile")
    north = lax.rem(tile, 2) == 1
    half = (ROWS - 4) // 2
    total = dot_rows([inner_ref[step : step + half] for step in range(3)], w2_ref)

    per_tile = ROWS * QW
    own = blocks_ref[...] - tile * per_tile
    hit = (frames_ref[...] == frame) & (own >= 0) & (own < per_tile)
    found = jnp.where(hit, own, 0).astype(jnp.float32)
    picks = [jnp.max(found[g : g + 1]).astype(jnp.int32) for g in range(FRAMES)]

    def second_rows(total, rows):
        for k, row in enumerate(rows):
            if 0 < row < ROWS - 1:
                base = middle_ref[row - 1]
            else:
                base = side_middle_ref[1 if row == 0 else 2]
            out = base.astype(jnp.float32) + total[k * W : (k + 1) * W]
            out = out.astype(jnp.bfloat16)
            refined_ref[row] = out
            wide_ref[row * W : (row + 1) * W] = out.astype(jnp.float32)

    def send(k, start, count):
        rows = pl.ds(start, count)
        copy = pltpu.make_async_copy(refined_ref.at[rows], refined_hbm.at[rows], sems.at[k])
        copy.start()
        return copy

    g1 = g1_ref[...] * 0.5
    g2 = g2_ref[...] * 0.5
    low, high = [], []
    for k in range(2):
        near = near_ref[k].astype(jnp.float32)
        away = away_ref[k].astype(jnp.float32)
        low.append(jnp.where(north, near, away))
        high.append(jnp.where(north, away, near))
    for k in range(2):
        store_windows(silu_norm(low[k], g1), first_ref, k)
        first_ref[2 + k] = sides_ref[k]
        first_ref[4 + k] = sides_ref[2 + k]
        store_windows(silu_norm(high[k], g1), first_ref, 6 + k)
        second_ref[2 + k] = inner_ref[k]
        second_ref[4 + k] = inner_ref[INNER - 2 + k]
    edges = dot_rows(
        [
            jnp.concatenate([first_ref[step : step + 2], first_ref[4 + step : 6 + step]], 0)
            for step in range(3)
        ],
        w1_ref,
    )
    second_rows(total, range(2, 2 + half))
    copies = [send(0, 2, half)]
    total = dot_rows([inner_ref[half + step : 2 * half + step] for step in range(3)], w2_ref)

    bases = [low[1], base_ref[0].astype(jnp.float32), base_ref[1].astype(jnp.float32), high[0]]
    places = [0, 1, 6, 7]
    for k in range(4):
        middle = bases[k] + edges[k * W : (k + 1) * W]
        act = silu_norm(middle, g2)
        if k == 0:
            act = jnp.where(tile > 0, act, 0.0)
        if k == 3:
            act = jnp.where(tile < TILES - 1, act, 0.0)
        side_middle_ref[k] = middle.astype(jnp.bfloat16)
        store_windows(act, second_ref, places[k])
    edges = dot_rows(
        [
            jnp.concatenate([second_ref[step : step + 2], second_ref[4 + step : 6 + step]], 0)
            for step in range(3)
        ],
        w2_ref,
    )
    second_rows(total, range(2 + half, ROWS - 2))
    copies.append(send(1, 2 + half, half))
    second_rows(edges, [0, 1, ROWS - 2, ROWS - 1])
    copies += [send(2, 0, 2), send(3, ROWS - 2, 2)]

    gk = gk_ref[...]
    for g in range(FRAMES):
        at = pl.multiple_of(picks[g] * BT, 8)
        block = normalized(wide_ref[pl.ds(at, BT)], gk)
        picked_ref[g] = block.astype(jnp.bfloat16)
    for copy in copies:
        copy.wait()


def outer_call(near, away, inner):
    return pl.pallas_call(
        outer_kernel,
        name="outer_rows",
        out_shape=(
            jax.ShapeDtypeStruct((ROWS, W, C), jnp.bfloat16),
            jax.ShapeDtypeStruct((FRAMES, BT, C), jnp.bfloat16),
        ),
        in_specs=[VMEM] * 13,
        out_specs=(pl.BlockSpec(memory_space=pltpu.HBM), VMEM),
        scratch_shapes=[
            pltpu.VMEM((ROWS, W, C), jnp.bfloat16),
            pltpu.VMEM((8, W, 3 * C), jnp.bfloat16),
            pltpu.VMEM((4, W, C), jnp.bfloat16),
            pltpu.VMEM((8, W, 3 * C), jnp.bfloat16),
            pltpu.VMEM((ROWS * W, C), jnp.float32),
            pltpu.SemaphoreType.DMA((4,)),
        ],
        compiler_params=pltpu.CompilerParams(vmem_limit_bytes=28 * 1024 * 1024),
        cost_estimate=pl.CostEstimate(
            flops=2 * 9 * C * C * W * (ROWS + 4), bytes_accessed=4 << 20, transcendentals=0
        ),
    )(near, away, *inner)


def query_kernel(q_ref, wk_ref, frames_ref, blocks_ref, high_ref, low_ref, bias_ref):
    frame = lax.axis_index("frames")
    tile = lax.axis_index("tile")
    per_tile = ROWS * QW
    row = lax.broadcasted_iota(jnp.int32, frames_ref.shape, 0)
    source = frames_ref[...] * TILES + lax.shift_right_arithmetic(blocks_ref[...], 6)
    source = jnp.where((row == frame) & (frames_ref[...] >= 0), source, -1)
    source = jnp.max(source.astype(jnp.float32), axis=0, keepdims=True)
    sources = FRAMES * TILES
    number = lax.broadcasted_iota(jnp.int32, (sources, source.shape[1]), 0).astype(jnp.float32)
    listed = jnp.max(jnp.where(source == number, 1.0, 0.0), axis=1, keepdims=True)
    tokens = FRAMES * BT
    place = lax.broadcasted_iota(jnp.int32, (sources, tokens), 1)
    of_frame = lax.shift_right_logical(place * 205, 13)
    number = lax.broadcasted_iota(jnp.int32, (sources, tokens), 0)
    wide = jnp.broadcast_to(listed, (sources, tokens))
    depth, core = lax.div(tile, 2), lax.rem(tile, 2)
    odd = lax.rem(depth, 2) == 1
    even_side = jnp.where(odd, depth - 1, depth + 1)
    odd_side = lax.rem(jnp.where(odd, depth + 1, depth + 3), 4)
    planes = {"own": depth, "x": even_side, "y": odd_side, "far": lax.rem(depth + 2, 4)}
    for k, (plane, other) in enumerate(ORDER):
        at = 2 * planes[plane] + (1 - core if other else core)
        match = jnp.where(number == of_frame * TILES + at, wide, 0.0)
        there = jnp.max(match, axis=0, keepdims=True)
        bias_ref[k : k + 1] = jnp.where(there > 0.5, 0.0, NEGATIVE)

    scale = LOG2E / HD**0.5
    for h in range(HEADS):
        cols = slice(h * HD, (h + 1) * HD)
        turned = lax.dot_general(
            q_ref[:, cols], wk_ref[:, cols], (((1,), (1,)), ((), ())),
            preferred_element_type=jnp.float32,
        ) * scale
        high = turned.astype(jnp.bfloat16)
        high_ref[h * Q_DEV : (h + 1) * Q_DEV] = high
        low_ref[h * Q_DEV : (h + 1) * Q_DEV] = (turned - high.astype(jnp.float32)).astype(
            jnp.bfloat16
        )


ORDER = (
    ("own", 0), ("own", 1), ("x", 0), ("y", 0), ("x", 1), ("y", 1), ("far", 0), ("far", 1),
)


def query_call(queries, key_weight, frame_ids, block_ids):
    shape = jax.ShapeDtypeStruct((QROWS, C), jnp.bfloat16)
    return pl.pallas_call(
        query_kernel,
        name="turn_queries",
        out_shape=(shape, shape, jax.ShapeDtypeStruct((TILES, FRAMES * BT), jnp.float32)),
        in_specs=[VMEM] * 4,
        out_specs=(VMEM,) * 3,
        compiler_params=pltpu.CompilerParams(vmem_limit_bytes=16 * 1024 * 1024),
        cost_estimate=pl.CostEstimate(
            flops=2 * QROWS * HD * C, bytes_accessed=3 << 20, transcendentals=0
        ),
    )(queries, key_weight, frame_ids, block_ids)


BLOCK = 256
SLAB = 32


def attend_kernel(first, last, parts, chunk, *refs):
    refs = list(refs)
    qh_ref, ql_ref = refs[:2]
    x_refs = refs[2 : 2 + parts]
    bias_ref = refs[2 + parts]
    refs = refs[3 + parts :]
    if not first:
        m_in, l_in, acc_in = refs[:3]
        refs = refs[3:]
    if last:
        wv_ref, out_ref = refs[:2]
        refs = refs[2:]
    else:
        m_out, l_out, acc_out = refs[:3]
        refs = refs[3:]
    x_ref, s_ref, p_ref = refs
    tokens = x_ref.shape[0]
    at = 0
    for part in x_refs:
        size = part.shape[0] * part.shape[1]
        x_ref[at : at + size] = part[...].reshape(size, C)
        at += size
    bias = jnp.concatenate([bias_ref[2 * chunk : 2 * chunk + 1], bias_ref[2 * chunk + 1 : 2 * chunk + 2]], 1)

    def scores(block, slot):
        rows = slice(block * BLOCK, (block + 1) * BLOCK)
        dims = (((1,), (1,)), ((), ()))
        s_ref[slot] = lax.dot_general(
            qh_ref[rows], x_ref[...], dims, preferred_element_type=jnp.float32
        ) + lax.dot_general(ql_ref[rows], x_ref[...], dims, preferred_element_type=jnp.float32)

    blocks = QROWS // BLOCK
    scores(0, 0)
    for block in range(blocks):
        slot = block % 2
        if block + 1 < blocks:
            scores(block + 1, 1 - slot)
        alphas = []
        sums = []
        for slab in range(BLOCK // SLAB):
            own = slice(slab * SLAB, (slab + 1) * SLAB)
            rows = slice(block * BLOCK + slab * SLAB, block * BLOCK + (slab + 1) * SLAB)
            s = s_ref[slot, own] + bias
            peak = jnp.max(s, axis=-1, keepdims=True)
            if not first:
                old = m_in[rows, 0:1]
                peak = jnp.maximum(peak, old)
                alphas.append(jnp.exp2(old - peak))
            p = jnp.exp2(s - peak)
            total = jnp.sum(p, axis=-1, keepdims=True)
            if not first:
                total = total + alphas[-1] * l_in[rows, 0:1]
            p_ref[slot, own] = p.astype(jnp.bfloat16)
            if last:
                sums.append(total)
            else:
                m_out[rows] = jnp.broadcast_to(peak, (SLAB, 128))
                l_out[rows] = jnp.broadcast_to(total, (SLAB, 128))
        rows = slice(block * BLOCK, (block + 1) * BLOCK)
        mixed = jnp.dot(p_ref[slot], x_ref[...], preferred_element_type=jnp.float32)
        if not first:
            mixed = mixed + jnp.concatenate(alphas, 0) * acc_in[rows]
        if not last:
            acc_out[rows] = mixed
        else:
            mixed = mixed / jnp.concatenate(sums, 0)
            high = mixed.astype(jnp.bfloat16)
            low = (mixed - high.astype(jnp.float32)).astype(jnp.bfloat16)
            for k in range(BLOCK // Q_DEV):
                h = block * (BLOCK // Q_DEV) + k
                cols = slice(h * HD, (h + 1) * HD)
                own = slice(k * Q_DEV, (k + 1) * Q_DEV)
                both = jnp.concatenate([high[own], low[own]], 0)
                value = jnp.dot(both, wv_ref[:, cols], preferred_element_type=jnp.float32)
                out_ref[:, cols] = (value[:Q_DEV] + value[Q_DEV:]).astype(jnp.bfloat16)


def attend_call(qh, ql, parts, bias, chunk, state=None, value_weight=None):
    first = state is None
    last = value_weight is not None
    tokens = sum(part.shape[0] * part.shape[1] for part in parts)
    operands = [qh, ql, *parts, bias]
    aliases = {}
    if not first:
        if not last:
            aliases = {len(operands) + k: k for k in range(3)}
        operands += list(state)
    if last:
        operands.append(value_weight)
        out_shape = jax.ShapeDtypeStruct((Q_DEV, HEADS * HD), jnp.bfloat16)
        out_specs = VMEM
    else:
        stat = jax.ShapeDtypeStruct((QROWS, 128), jnp.float32)
        out_shape = (stat, stat, jax.ShapeDtypeStruct((QROWS, C), jnp.float32))
        out_specs = (VMEM, VMEM, VMEM)
    return pl.pallas_call(
        functools.partial(attend_kernel, first, last, len(parts), chunk),
        name="attend",
        out_shape=out_shape,
        in_specs=[VMEM] * len(operands),
        out_specs=out_specs,
        input_output_aliases=aliases,
        scratch_shapes=[
            pltpu.VMEM((tokens, C), jnp.bfloat16),
            pltpu.VMEM((2, BLOCK, tokens), jnp.float32),
            pltpu.VMEM((2, BLOCK, tokens), jnp.bfloat16),
        ],
        compiler_params=pltpu.CompilerParams(vmem_limit_bytes=24 * 1024 * 1024),
        cost_estimate=pl.CostEstimate(
            flops=6 * QROWS * C * tokens, bytes_accessed=6 << 20, transcendentals=QROWS * tokens
        ),
    )(*operands)


def core_swap(x):
    return lax.ppermute(x, "tile", [(t, t ^ 1) for t in range(TILES)])


def partner_plane(z, odd):
    return z ^ 1 if not odd else ((z + 1) % 4 if z % 2 else (z + 3) % 4)


def plane_swap(x, odds):
    pairs = [(t, 2 * partner_plane(t // 2, odds[t % 2]) + t % 2) for t in range(TILES)]
    return lax.ppermute(x, "tile", pairs)


def local(
    latents, conv_first, conv_second, gain_first, gain_second, gain_key,
    queries, key_weight, value_weight, frame_ids, block_ids, counts,
):
    core = lax.rem(lax.axis_index("tile"), 2)
    own = latents[0]
    near = lax.dynamic_slice_in_dim(own, (ROWS - 2) * (1 - core), 2, 0)
    away = lax.dynamic_slice_in_dim(own, (ROWS - 2) * core, 2, 0)
    near = core_swap(near)
    across = [(t, t + 1 if t % 2 else t - 1) for t in range(1, TILES - 1)]
    away = lax.ppermute(away, "tile", across)

    stay = functools.partial(pltpu.with_memory_space_constraint, memory_space=pltpu.HBM)
    inner = inner_call(
        stay(own),
        stay(conv_first.reshape(3, 3 * C, C)), stay(conv_second.reshape(3, 3 * C, C)),
        stay(gain_first[None]), stay(gain_second[None]), stay(gain_key[None]),
        stay(frame_ids), stay(block_ids),
    )
    refined, picked = outer_call(near, away, inner)
    qh, ql, bias = query_call(queries, key_weight, inner[9], inner[10])
    mine = lax.all_to_all(picked, "frames", split_axis=0, concat_axis=0, tiled=True)
    partner = core_swap(mine)
    even_side = plane_swap(mine, (False, False))
    odd_side = plane_swap(mine, (True, True))
    state = attend_call(qh, ql, (mine, partner), bias, 0)
    even_side, odd_side, state = lax.optimization_barrier((even_side, odd_side, state))
    far = plane_swap(jnp.where(core == 0, even_side, odd_side), (True, False))
    even_swap = core_swap(even_side)
    odd_swap = core_swap(odd_side)
    state = attend_call(qh, ql, (even_side, odd_side), bias, 1, state)
    state = attend_call(qh, ql, (even_swap, odd_swap), bias, 2, state)
    far, state = lax.optimization_barrier((far, state))
    far_swap = core_swap(far)
    attended = attend_call(qh, ql, (far, far_swap), bias, 3, state, value_weight)
    return (refined[None], attended)


def solution(mesh):
    in_specs = (
        P("frames", "tile", None, None),
        P(), P(), P(), P(), P(),
        P(("frames", "tile"), None),
        P(), P(), P(), P(), P(),
    )
    out_specs = (P("frames", "tile", None, None), P(("frames", "tile"), None))
    return jax.shard_map(local, mesh=mesh, in_specs=in_specs, out_specs=out_specs, check_vma=False)
```

```python
import functools

import jax
import jax.numpy as jnp
from jax import lax
from jax.experimental import pallas as pl
from jax.experimental.pallas import tpu as pltpu
from jax.sharding import PartitionSpec as P

C = 256
HEADS = 20
HD = 128
QW = 4
BT = 40
W = 160
ROWS = 16
Q_DEV = 64
FRAMES = 16
TILES = 8
QROWS = HEADS * Q_DEV
EPSILON = 1e-06
NEGATIVE = -1e30
LOG2E = 1.4426950408889634
VMEM = pl.BlockSpec(memory_space=pltpu.VMEM)
SMEM = pl.BlockSpec(memory_space=pltpu.SMEM)


def normalized(wide, gain):
    mean_square = jnp.mean(wide * wide, axis=-1, keepdims=True)
    return wide * lax.rsqrt(mean_square + EPSILON) * gain


def store_windows(act, dst_ref, row):
    column = lax.broadcasted_iota(jnp.int32, (8, C), 0)
    left = pltpu.roll(act, 1, 0)
    left = jnp.concatenate([jnp.where(column == 0, 0.0, left[:8]), left[8:]], 0)
    right = pltpu.roll(act, W - 1, 0)
    right = jnp.concatenate([right[: W - 8], jnp.where(column == 7, 0.0, right[W - 8 :])], 0)
    dst_ref[row, :, 0:C] = left.astype(jnp.bfloat16)
    dst_ref[row, :, C : 2 * C] = act.astype(jnp.bfloat16)
    dst_ref[row, :, 2 * C : 3 * C] = right.astype(jnp.bfloat16)


def silu_norm(wide, half_gain):
    half = normalized(wide, half_gain)
    return half + half * jnp.tanh(half)


def dot_rows(windows, weight_ref):
    total = None
    for step, window in enumerate(windows):
        part = jnp.dot(
            window.reshape(-1, 3 * C), weight_ref[step], preferred_element_type=jnp.float32
        )
        total = part if total is None else total + part
    return total


INNER = ROWS - 2


def inner_kernel(
    x_hbm, w1_hbm, w2_hbm, g1_hbm, g2_hbm, gk_hbm, frames_hbm, blocks_hbm,
    second_ref, middle_ref, sides_ref, base_ref, w1_ref, w2_ref,
    g1_ref, g2_ref, gk_ref, frames_ref, blocks_ref,
    x_ref, first_ref, sems,
):
    chunk = ROWS // 4
    pairs = [(g1_hbm, g1_ref), (g2_hbm, g2_ref)]
    for k in range(4):
        own = pl.ds(k * chunk, chunk)
        pairs.append((x_hbm.at[own], x_ref.at[own]))
    pairs += [
        (w1_hbm, w1_ref), (w2_hbm, w2_ref), (gk_hbm, gk_ref),
        (frames_hbm, frames_ref), (blocks_hbm, blocks_ref),
    ]
    copies = [
        pltpu.make_async_copy(src, dst, sems.at[k]) for k, (src, dst) in enumerate(pairs)
    ]
    for k in (2, 0, 3, 4, 5, 1, 6):
        copies[k].start()
    copies[0].wait()
    g1 = g1_ref[...] * 0.5

    def first_rows(rows):
        for row in rows:
            store_windows(silu_norm(x_ref[row].astype(jnp.float32), g1), first_ref, row)

    def middle_rows(rows):
        start, count = rows[0], len(rows)
        return dot_rows(
            [first_ref[start + step : start + step + count] for step in range(3)], w1_ref
        )

    def second_rows(rows, total, g2):
        for k, row in enumerate(rows):
            middle = x_ref[row + 1].astype(jnp.float32) + total[k * W : (k + 1) * W]
            middle_ref[row] = middle.astype(jnp.bfloat16)
            store_windows(silu_norm(middle, g2), second_ref, row)

    copies[2].wait()
    first_rows(range(0, chunk))
    for k in (3, 4, 5, 1, 6):
        copies[k].wait()
    later = copies[7:]
    for copy in later:
        copy.start()
    g2 = g2_ref[...] * 0.5
    first_rows(range(chunk, 7))
    parts = [range(0, 5), range(5, 10), range(10, INNER)]
    totals = [middle_rows(parts[0])]
    first_rows(range(7, 12))
    totals.append(middle_rows(parts[1]))
    first_rows(range(12, ROWS))
    second_rows(parts[0], totals[0], g2)
    totals.append(middle_rows(parts[2]))
    for k in range(2):
        sides_ref[k] = first_ref[k]
        sides_ref[2 + k] = first_ref[ROWS - 2 + k]
        base_ref[k] = x_ref[k * (ROWS - 1)]
    second_rows(parts[1], totals[1], g2)
    second_rows(parts[2], totals[2], g2)
    for copy in later:
        copy.wait()


def inner_call(latents, w1, w2, g1, g2, gk, frame_ids, block_ids):
    weight = jax.ShapeDtypeStruct((3, 3 * C, C), jnp.bfloat16)
    gain = jax.ShapeDtypeStruct((1, C), jnp.float32)
    table = jax.ShapeDtypeStruct(frame_ids.shape, jnp.int32)
    out_shape = (
        jax.ShapeDtypeStruct((INNER, W, 3 * C), jnp.bfloat16),
        jax.ShapeDtypeStruct((INNER, W, C), jnp.bfloat16),
        jax.ShapeDtypeStruct((4, W, 3 * C), jnp.bfloat16),
        jax.ShapeDtypeStruct((2, W, C), jnp.bfloat16),
        weight, weight, gain, gain, gain, table, table,
    )
    return pl.pallas_call(
        inner_kernel,
        name="inner_rows",
        out_shape=out_shape,
        in_specs=[pl.BlockSpec(memory_space=pltpu.HBM)] * 8,
        out_specs=(VMEM,) * len(out_shape),
        scratch_shapes=[
            pltpu.VMEM((ROWS, W, C), jnp.bfloat16),
            pltpu.VMEM((ROWS, W, 3 * C), jnp.bfloat16),
            pltpu.SemaphoreType.DMA((11,)),
        ],
        compiler_params=pltpu.CompilerParams(vmem_limit_bytes=28 * 1024 * 1024),
        cost_estimate=pl.CostEstimate(
            flops=2 * 9 * C * C * W * INNER, bytes_accessed=4 << 20, transcendentals=0
        ),
    )(latents, w1, w2, g1, g2, gk, frame_ids, block_ids)


def outer_kernel(
    near_ref, away_ref, inner_ref, middle_ref, sides_ref, base_ref, w1_ref, w2_ref,
    g1_ref, g2_ref, gk_ref, frames_ref, blocks_ref,
    refined_hbm, picked_ref,
    refined_ref, first_ref, side_middle_ref, second_ref, wide_ref, sems,
):
    frame = lax.axis_index("frames")
    tile = lax.axis_index("tile")
    north = lax.rem(tile, 2) == 1
    half = (ROWS - 4) // 2
    total = dot_rows([inner_ref[step : step + half] for step in range(3)], w2_ref)

    per_tile = ROWS * QW
    own = blocks_ref[...] - tile * per_tile
    hit = (frames_ref[...] == frame) & (own >= 0) & (own < per_tile)
    found = jnp.where(hit, own, 0).astype(jnp.float32)
    picks = [jnp.max(found[g : g + 1]).astype(jnp.int32) for g in range(FRAMES)]

    def second_rows(total, rows):
        for k, row in enumerate(rows):
            if 0 < row < ROWS - 1:
                base = middle_ref[row - 1]
            else:
                base = side_middle_ref[1 if row == 0 else 2]
            out = base.astype(jnp.float32) + total[k * W : (k + 1) * W]
            out = out.astype(jnp.bfloat16)
            refined_ref[row] = out
            wide_ref[row * W : (row + 1) * W] = out.astype(jnp.float32)

    def send(k, start, count):
        rows = pl.ds(start, count)
        copy = pltpu.make_async_copy(refined_ref.at[rows], refined_hbm.at[rows], sems.at[k])
        copy.start()
        return copy

    g1 = g1_ref[...] * 0.5
    g2 = g2_ref[...] * 0.5
    low, high = [], []
    for k in range(2):
        near = near_ref[k].astype(jnp.float32)
        away = away_ref[k].astype(jnp.float32)
        low.append(jnp.where(north, near, away))
        high.append(jnp.where(north, away, near))
    for k in range(2):
        store_windows(silu_norm(low[k], g1), first_ref, k)
        first_ref[2 + k] = sides_ref[k]
        first_ref[4 + k] = sides_ref[2 + k]
        store_windows(silu_norm(high[k], g1), first_ref, 6 + k)
        second_ref[2 + k] = inner_ref[k]
        second_ref[4 + k] = inner_ref[INNER - 2 + k]
    edges = dot_rows(
        [
            jnp.concatenate([first_ref[step : step + 2], first_ref[4 + step : 6 + step]], 0)
            for step in range(3)
        ],
        w1_ref,
    )
    second_rows(total, range(2, 2 + half))
    copies = [send(0, 2, half)]
    total = dot_rows([inner_ref[half + step : 2 * half + step] for step in range(3)], w2_ref)

    bases = [low[1], base_ref[0].astype(jnp.float32), base_ref[1].astype(jnp.float32), high[0]]
    places = [0, 1, 6, 7]
    for k in range(4):
        middle = bases[k] + edges[k * W : (k + 1) * W]
        act = silu_norm(middle, g2)
        if k == 0:
            act = jnp.where(tile > 0, act, 0.0)
        if k == 3:
            act = jnp.where(tile < TILES - 1, act, 0.0)
        side_middle_ref[k] = middle.astype(jnp.bfloat16)
        store_windows(act, second_ref, places[k])
    edges = dot_rows(
        [
            jnp.concatenate([second_ref[step : step + 2], second_ref[4 + step : 6 + step]], 0)
            for step in range(3)
        ],
        w2_ref,
    )
    second_rows(total, range(2 + half, ROWS - 2))
    copies.append(send(1, 2 + half, half))
    second_rows(edges, [0, 1, ROWS - 2, ROWS - 1])
    copies += [send(2, 0, 2), send(3, ROWS - 2, 2)]

    gk = gk_ref[...]
    for g in range(FRAMES):
        at = pl.multiple_of(picks[g] * BT, 8)
        block = normalized(wide_ref[pl.ds(at, BT)], gk)
        picked_ref[g] = block.astype(jnp.bfloat16)
    for copy in copies:
        copy.wait()


def outer_call(near, away, inner):
    return pl.pallas_call(
        outer_kernel,
        name="outer_rows",
        out_shape=(
            jax.ShapeDtypeStruct((ROWS, W, C), jnp.bfloat16),
            jax.ShapeDtypeStruct((FRAMES, BT, C), jnp.bfloat16),
        ),
        in_specs=[VMEM] * 13,
        out_specs=(pl.BlockSpec(memory_space=pltpu.HBM), VMEM),
        scratch_shapes=[
            pltpu.VMEM((ROWS, W, C), jnp.bfloat16),
            pltpu.VMEM((8, W, 3 * C), jnp.bfloat16),
            pltpu.VMEM((4, W, C), jnp.bfloat16),
            pltpu.VMEM((8, W, 3 * C), jnp.bfloat16),
            pltpu.VMEM((ROWS * W, C), jnp.float32),
            pltpu.SemaphoreType.DMA((4,)),
        ],
        compiler_params=pltpu.CompilerParams(vmem_limit_bytes=28 * 1024 * 1024),
        cost_estimate=pl.CostEstimate(
            flops=2 * 9 * C * C * W * (ROWS + 4), bytes_accessed=4 << 20, transcendentals=0
        ),
    )(near, away, *inner)


def query_kernel(q_ref, wk_ref, frames_ref, blocks_ref, high_ref, low_ref, bias_ref):
    frame = lax.axis_index("frames")
    tile = lax.axis_index("tile")
    per_tile = ROWS * QW
    row = lax.broadcasted_iota(jnp.int32, frames_ref.shape, 0)
    source = frames_ref[...] * TILES + lax.shift_right_arithmetic(blocks_ref[...], 6)
    source = jnp.where((row == frame) & (frames_ref[...] >= 0), source, -1)
    source = jnp.max(source.astype(jnp.float32), axis=0, keepdims=True)
    sources = FRAMES * TILES
    number = lax.broadcasted_iota(jnp.int32, (sources, source.shape[1]), 0).astype(jnp.float32)
    listed = jnp.max(jnp.where(source == number, 1.0, 0.0), axis=1, keepdims=True)
    tokens = FRAMES * BT
    place = lax.broadcasted_iota(jnp.int32, (sources, tokens), 1)
    of_frame = lax.shift_right_logical(place * 205, 13)
    number = lax.broadcasted_iota(jnp.int32, (sources, tokens), 0)
    wide = jnp.broadcast_to(listed, (sources, tokens))
    depth, core = lax.div(tile, 2), lax.rem(tile, 2)
    odd = lax.rem(depth, 2) == 1
    even_side = jnp.where(odd, depth - 1, depth + 1)
    odd_side = lax.rem(jnp.where(odd, depth + 1, depth + 3), 4)
    planes = {"own": depth, "x": even_side, "y": odd_side, "far": lax.rem(depth + 2, 4)}
    for k, (plane, other) in enumerate(ORDER):
        at = 2 * planes[plane] + (1 - core if other else core)
        match = jnp.where(number == of_frame * TILES + at, wide, 0.0)
        there = jnp.max(match, axis=0, keepdims=True)
        bias_ref[k : k + 1] = jnp.where(there > 0.5, 0.0, NEGATIVE)

    scale = LOG2E / HD**0.5
    for h in range(HEADS):
        cols = slice(h * HD, (h + 1) * HD)
        turned = lax.dot_general(
            q_ref[:, cols], wk_ref[:, cols], (((1,), (1,)), ((), ())),
            preferred_element_type=jnp.float32,
        ) * scale
        high = turned.astype(jnp.bfloat16)
        high_ref[h * Q_DEV : (h + 1) * Q_DEV] = high
        low_ref[h * Q_DEV : (h + 1) * Q_DEV] = (turned - high.astype(jnp.float32)).astype(
            jnp.bfloat16
        )


ORDER = (
    ("own", 0), ("own", 1), ("x", 0), ("y", 0), ("x", 1), ("y", 1), ("far", 0), ("far", 1),
)


def query_call(queries, key_weight, frame_ids, block_ids):
    shape = jax.ShapeDtypeStruct((QROWS, C), jnp.bfloat16)
    return pl.pallas_call(
        query_kernel,
        name="turn_queries",
        out_shape=(shape, shape, jax.ShapeDtypeStruct((TILES, FRAMES * BT), jnp.float32)),
        in_specs=[VMEM] * 4,
        out_specs=(VMEM,) * 3,
        compiler_params=pltpu.CompilerParams(vmem_limit_bytes=16 * 1024 * 1024),
        cost_estimate=pl.CostEstimate(
            flops=2 * QROWS * HD * C, bytes_accessed=3 << 20, transcendentals=0
        ),
    )(queries, key_weight, frame_ids, block_ids)


BLOCK = 256
SLAB = 32


def attend_kernel(first, last, parts, chunk, *refs):
    refs = list(refs)
    qh_ref, ql_ref = refs[:2]
    x_refs = refs[2 : 2 + parts]
    bias_ref = refs[2 + parts]
    refs = refs[3 + parts :]
    if not first:
        m_in, l_in, acc_in = refs[:3]
        refs = refs[3:]
    if last:
        wv_ref, out_ref = refs[:2]
        refs = refs[2:]
    else:
        m_out, l_out, acc_out = refs[:3]
        refs = refs[3:]
    x_ref, s_ref, p_ref = refs
    tokens = x_ref.shape[0]
    at = 0
    for part in x_refs:
        size = part.shape[0] * part.shape[1]
        x_ref[at : at + size] = part[...].reshape(size, C)
        at += size
    bias = jnp.concatenate([bias_ref[2 * chunk : 2 * chunk + 1], bias_ref[2 * chunk + 1 : 2 * chunk + 2]], 1)

    def scores(block, slot):
        rows = slice(block * BLOCK, (block + 1) * BLOCK)
        dims = (((1,), (1,)), ((), ()))
        s_ref[slot] = lax.dot_general(
            qh_ref[rows], x_ref[...], dims, preferred_element_type=jnp.float32
        ) + lax.dot_general(ql_ref[rows], x_ref[...], dims, preferred_element_type=jnp.float32)

    blocks = QROWS // BLOCK
    scores(0, 0)
    for block in range(blocks):
        slot = block % 2
        if block + 1 < blocks:
            scores(block + 1, 1 - slot)
        alphas = []
        peaks = []
        sums = []
        slabs = range(block * BLOCK, (block + 1) * BLOCK, SLAB)
        if not first:
            old_peaks = [m_in[at : at + SLAB, 0:1] for at in slabs]
            old_sums = [l_in[at : at + SLAB, 0:1] for at in slabs]
        for slab in range(BLOCK // SLAB):
            own = slice(slab * SLAB, (slab + 1) * SLAB)
            s = s_ref[slot, own] + bias
            peak = jnp.max(s, axis=-1, keepdims=True)
            if not first:
                old = old_peaks[slab]
                peak = jnp.maximum(peak, old)
                alphas.append(jnp.exp2(old - peak))
            p = jnp.exp2(s - peak)
            total = jnp.sum(p, axis=-1, keepdims=True)
            if not first:
                total = total + alphas[-1] * old_sums[slab]
            p_ref[slot, own] = p.astype(jnp.bfloat16)
            peaks.append(peak)
            sums.append(total)
        if not last:
            for slab, at in enumerate(slabs):
                m_out[at : at + SLAB] = jnp.broadcast_to(peaks[slab], (SLAB, 128))
                l_out[at : at + SLAB] = jnp.broadcast_to(sums[slab], (SLAB, 128))
        rows = slice(block * BLOCK, (block + 1) * BLOCK)
        mixed = jnp.dot(p_ref[slot], x_ref[...], preferred_element_type=jnp.float32)
        if not first:
            mixed = mixed + jnp.concatenate(alphas, 0) * acc_in[rows]
        if not last:
            acc_out[rows] = mixed
        else:
            mixed = mixed / jnp.concatenate(sums, 0)
            high = mixed.astype(jnp.bfloat16)
            low = (mixed - high.astype(jnp.float32)).astype(jnp.bfloat16)
            for k in range(BLOCK // Q_DEV):
                h = block * (BLOCK // Q_DEV) + k
                cols = slice(h * HD, (h + 1) * HD)
                own = slice(k * Q_DEV, (k + 1) * Q_DEV)
                both = jnp.concatenate([high[own], low[own]], 0)
                value = jnp.dot(both, wv_ref[:, cols], preferred_element_type=jnp.float32)
                out_ref[:, cols] = (value[:Q_DEV] + value[Q_DEV:]).astype(jnp.bfloat16)


def attend_call(qh, ql, parts, bias, chunk, state=None, value_weight=None):
    first = state is None
    last = value_weight is not None
    tokens = sum(part.shape[0] * part.shape[1] for part in parts)
    operands = [qh, ql, *parts, bias]
    aliases = {}
    if not first:
        if not last:
            aliases = {}
        operands += list(state)
    if last:
        operands.append(value_weight)
        out_shape = jax.ShapeDtypeStruct((Q_DEV, HEADS * HD), jnp.bfloat16)
        out_specs = VMEM
    else:
        stat = jax.ShapeDtypeStruct((QROWS, 128), jnp.float32)
        out_shape = (stat, stat, jax.ShapeDtypeStruct((QROWS, C), jnp.float32))
        out_specs = (VMEM, VMEM, VMEM)
    return pl.pallas_call(
        functools.partial(attend_kernel, first, last, len(parts), chunk),
        name="attend",
        out_shape=out_shape,
        in_specs=[VMEM] * len(operands),
        out_specs=out_specs,
        input_output_aliases=aliases,
        scratch_shapes=[
            pltpu.VMEM((tokens, C), jnp.bfloat16),
            pltpu.VMEM((2, BLOCK, tokens), jnp.float32),
            pltpu.VMEM((2, BLOCK, tokens), jnp.bfloat16),
        ],
        compiler_params=pltpu.CompilerParams(vmem_limit_bytes=24 * 1024 * 1024),
        cost_estimate=pl.CostEstimate(
            flops=6 * QROWS * C * tokens, bytes_accessed=6 << 20, transcendentals=QROWS * tokens
        ),
    )(*operands)


def core_swap(x):
    return lax.ppermute(x, "tile", [(t, t ^ 1) for t in range(TILES)])


def partner_plane(z, odd):
    return z ^ 1 if not odd else ((z + 1) % 4 if z % 2 else (z + 3) % 4)


def plane_swap(x, odds):
    pairs = [(t, 2 * partner_plane(t // 2, odds[t % 2]) + t % 2) for t in range(TILES)]
    return lax.ppermute(x, "tile", pairs)


def local(
    latents, conv_first, conv_second, gain_first, gain_second, gain_key,
    queries, key_weight, value_weight, frame_ids, block_ids, counts,
):
    core = lax.rem(lax.axis_index("tile"), 2)
    own = latents[0]
    near = lax.dynamic_slice_in_dim(own, (ROWS - 2) * (1 - core), 2, 0)
    away = lax.dynamic_slice_in_dim(own, (ROWS - 2) * core, 2, 0)
    near = core_swap(near)
    across = [(t, t + 1 if t % 2 else t - 1) for t in range(1, TILES - 1)]
    away = lax.ppermute(away, "tile", across)

    stay = functools.partial(pltpu.with_memory_space_constraint, memory_space=pltpu.HBM)
    inner = inner_call(
        stay(own),
        stay(conv_first.reshape(3, 3 * C, C)), stay(conv_second.reshape(3, 3 * C, C)),
        stay(gain_first[None]), stay(gain_second[None]), stay(gain_key[None]),
        stay(frame_ids), stay(block_ids),
    )
    refined, picked = outer_call(near, away, inner)
    qh, ql, bias = query_call(queries, key_weight, inner[9], inner[10])
    mine = lax.all_to_all(picked, "frames", split_axis=0, concat_axis=0, tiled=True)
    partner = core_swap(mine)
    even_side = plane_swap(mine, (False, False))
    odd_side = plane_swap(mine, (True, True))
    state = attend_call(qh, ql, (mine, partner), bias, 0)
    even_side, odd_side, state = lax.optimization_barrier((even_side, odd_side, state))
    far = plane_swap(jnp.where(core == 0, even_side, odd_side), (True, False))
    even_swap = core_swap(even_side)
    odd_swap = core_swap(odd_side)
    state = attend_call(qh, ql, (even_side, odd_side), bias, 1, state)
    state = attend_call(qh, ql, (even_swap, odd_swap), bias, 2, state)
    far, state = lax.optimization_barrier((far, state))
    far_swap = core_swap(far)
    attended = attend_call(qh, ql, (far, far_swap), bias, 3, state, value_weight)
    return (refined[None], attended)


def solution(mesh):
    in_specs = (
        P("frames", "tile", None, None),
        P(), P(), P(), P(), P(),
        P(("frames", "tile"), None),
        P(), P(), P(), P(), P(),
    )
    out_specs = (P("frames", "tile", None, None), P(("frames", "tile"), None))
    return jax.shard_map(local, mesh=mesh, in_specs=in_specs, out_specs=out_specs, check_vma=False)
```
